32 devices in a mesh: dp: 16 (over z, y, x), mp: 2 (over core).
Axes of the slice: x: 2, y: 2, z: 4, core: 2. Of those that a mesh axis runs over, the one named last changes fastest.
Arguments:
- attn: bfloat16 [6144, 1536], P('dp', 'mp'), may hold values from -6 to 6
- w_out: bfloat16 [1536, 1536], P('mp'), may hold values from -0.15625 to 0.15625
- resid: bfloat16 [6144, 1536], P('dp', 'mp'), may hold values from -6 to 6
- target: bfloat16 [6144, 1536], P('dp', 'mp'), may hold values from -6 to 6
- gate: float32 [48, 1536], P('dp', 'mp'), may hold values from -5 to 5
- bins: int32 [48], P('dp'), may hold values from 0 to 127
Outputs:
- grad_w_out: float32 [1536, 1536], P('dp', 'mp')
- grad_gate: float32 [48, 1536], P('dp', 'mp')
- bin_loss: float32 [128], replicated
The draws below stay inside these ranges and needn't reach their ends.
All inputs are finite; a program needn't handle non-finite values.
Results may differ from the reference program's by a relative error of at most 0.0008.
Values may be sent and summed in bfloat16 or wider, within the bound.
A program may use at most 64 MiB of HBM per device.

```python
import math
import jax
import jax.numpy as jnp
from jax import lax

D = 1536
NBINS = 128
SAMP_DEV = 3
TOK_SAMP = 128
SAMPLES = 48
TOKENS = 6144
N_DP = 16


def plant(entries, stream_key, low, top_value):
    place = [jax.random.randint(jax.random.fold_in(stream_key, axis), (), 0, length) for axis, length in enumerate(entries.shape)]
    widest = entries.shape.index(max(entries.shape))
    neighbour = place[:widest] + [(place[widest] + 1) % entries.shape[widest]] + place[widest + 1:]
    return entries.at[tuple(place)].set(low).at[tuple(neighbour)].set(top_value)


def block_scale(stream_key, dims, shards, low, largest):
    gain, own = 1.0, jax.random.fold_in(stream_key, 6)
    for axis_at, shards_of in shards:
        heights = jnp.exp(jax.random.uniform(jax.random.fold_in(own, axis_at), (shards_of,), jnp.float32, low / len(shards), largest / len(shards)))
        gain = gain * jnp.repeat(heights, dims[axis_at] // shards_of).reshape([-1 if axis == axis_at else 1 for axis in range(len(dims))])
    return gain


def centred(stream_key, dims, width, bound, pieces=(), held_as=jnp.bfloat16):
    values = width * jax.random.normal(stream_key, dims, jnp.float32)
    if pieces:
        values = values * block_scale(stream_key, dims, pieces, -0.22, 0.18)
    return jnp.clip(values, -bound, bound).astype(held_as)


def setup_inputs(seed: int = 0) -> dict:
    streams_of = jax.random.split(jax.random.key(seed), 7)
    return {
        "attn": centred(streams_of[0], (TOKENS, D), 1.0, 6.0, ((0, 16), (1, 2))),
        "w_out": centred(streams_of[1], (D, D), D ** -0.5, 0.15625, ((0, 2),)),
        "resid": centred(streams_of[2], (TOKENS, D), 1.0, 6.0, ((0, 16), (1, 2))),
        "target": centred(streams_of[3], (TOKENS, D), 1.0, 6.0, ((0, 16), (1, 2))),
        "gate": centred(streams_of[4], (SAMPLES, D), 1.0, 5.0, ((0, 16), (1, 2)), jnp.float32),
        "bins": plant(jax.random.randint(streams_of[5], (SAMPLES,), 0, NBINS), jax.random.fold_in(streams_of[5], 1), 0, NBINS - 1).astype(jnp.int32),
    }


LOSS_SCALE = 4096.0

def bin_weights():
    centre = (jnp.arange(NBINS).astype(jnp.float32) + 0.5) / NBINS
    logit = jnp.log(centre) - jnp.log(1.0 - centre)
    return jnp.exp(-0.5 * logit * logit) / (math.sqrt(2.0 * math.pi) * centre * (1.0 - centre))

def reference(attn, w_out, resid, target, gate, bins):
    bin_ids = jnp.arange(NBINS, dtype=jnp.int32)
    one_hot = (bins[:, None] == bin_ids[None, :]).astype(jnp.float32)
    counts = lax.optimization_barrier(jnp.sum(one_hot, axis=0))
    floored = jnp.maximum(counts, 1.0)
    weights = bin_weights()
    scale_bin = LOSS_SCALE * weights / floored
    coefficient = lax.optimization_barrier(jnp.sum(one_hot * scale_bin[None, :], axis=1)) * (2.0 / (TOK_SAMP * D))
    tok_rows = SAMP_DEV * TOK_SAMP
    attn_blocks = attn.reshape(N_DP, tok_rows, D)
    resid_blocks = resid.reshape(N_DP, tok_rows, D)
    target_blocks = target.reshape(N_DP, tok_rows, D)
    gate_blocks = gate.reshape(N_DP, SAMP_DEV, D)
    coef_blocks = coefficient.reshape(N_DP, SAMP_DEV)

    def step(total, inputs):
        attn_in, resid_in, target_in, gate_in, coef_in = inputs
        projected = jnp.dot(attn_in, w_out, preferred_element_type=jnp.float32).reshape(SAMP_DEV, TOK_SAMP, D)
        hidden = resid_in.reshape(SAMP_DEV, TOK_SAMP, D).astype(jnp.float32) + gate_in[:, None, :] * projected
        error_cube = hidden - target_in.reshape(SAMP_DEV, TOK_SAMP, D).astype(jnp.float32)
        sample_error = lax.optimization_barrier(jnp.sum(error_cube * error_cube, axis=(1, 2))) / (TOK_SAMP * D)
        d_hidden = coef_in[:, None, None] * error_cube
        grad_gate = lax.optimization_barrier(jnp.sum(d_hidden * projected, axis=1))
        d_proj = (d_hidden * gate_in[:, None, :]).astype(jnp.bfloat16).reshape(tok_rows, D)
        total = total + lax.dot_general(attn_in, d_proj, (((0,), (0,)), ((), ())), preferred_element_type=jnp.float32)
        return (total, (sample_error, grad_gate))
    start_total = jnp.zeros((D, D), jnp.float32)
    total, (errors, grads) = lax.scan(step, start_total, (attn_blocks, resid_blocks, target_blocks, gate_blocks, coef_blocks))
    sums = lax.optimization_barrier(jnp.sum(one_hot * errors.reshape(-1)[:, None], axis=0))
    bin_loss = weights * sums / floored
    return (total, grads.reshape(SAMPLES, D), bin_loss)
```

```python
import functools
import math

import jax
import jax.numpy as jnp
from jax import lax
from jax.experimental import pallas as pl
from jax.experimental.pallas import tpu as pltpu
from jax.sharding import PartitionSpec as P

NBINS = 128


LOSS_SCALE = 4096.0


def bin_weights():
    centre = (jnp.arange(NBINS).astype(jnp.float32) + 0.5) / NBINS
    logit = jnp.log(centre) - jnp.log(1.0 - centre)
    return jnp.exp(-0.5 * logit * logit) / (math.sqrt(2.0 * math.pi) * centre * (1.0 - centre))


def shards(attn, w_out, resid, target, gate, bins):
    samples = bins.shape[0]
    tok_rows = attn.shape[0]
    per_sample = tok_rows // samples
    full_width = w_out.shape[1]
    own_cols = resid.shape[1]
    bin_ids = jnp.arange(NBINS, dtype=jnp.int32)
    one_hot = (bins[:, None] == bin_ids[None, :]).astype(jnp.float32)
    local_counts = jnp.sum(one_hot, axis=0)
    weights = bin_weights()
    counts = lax.psum(local_counts, "dp")
    whole_attn = lax.all_gather(attn, "mp", axis=1, tiled=True)
    partial_value = jnp.dot(attn, w_out, preferred_element_type=jnp.float32)
    projected = lax.psum_scatter(partial_value, "mp", scatter_dimension=1, tiled=True)
    proj_cube = projected.reshape(samples, per_sample, own_cols)
    hidden = (
        resid.reshape(samples, per_sample, own_cols).astype(jnp.float32)
        + gate[:, None, :] * proj_cube
    )
    error_cube = hidden - target.reshape(samples, per_sample, own_cols).astype(jnp.float32)
    sample_error = jnp.sum(error_cube * error_cube, axis=(1, 2)) / (per_sample * full_width)
    bin_part = jnp.sum(one_hot * sample_error[:, None], axis=0)
    sums = lax.psum(bin_part, ("dp", "mp"))
    floored = jnp.maximum(counts, 1.0)
    scale_bin = LOSS_SCALE * weights / floored
    coefficient = jnp.sum(one_hot * scale_bin[None, :], axis=1) * (2.0 / (per_sample * full_width))
    d_hidden = coefficient[:, None, None] * error_cube
    grad_gate = jnp.sum(d_hidden * proj_cube, axis=1)
    d_proj = (d_hidden * gate[:, None, :]).astype(jnp.bfloat16).reshape(tok_rows, own_cols)
    full_grad = lax.dot_general(
        whole_attn, d_proj, (((0,), (0,)), ((), ())), preferred_element_type=jnp.float32
    )
    grad_out = lax.psum_scatter(full_grad, "dp", scatter_dimension=0, tiled=True)
    bin_loss = weights * sums / floored
    return (grad_out, grad_gate, bin_loss)


MESH = pl.DeviceIdType.MESH
LANES = 128
PLANE = 4


def fused_kernel(
    n, full_width,
    attn_h, w_h, resid_h, target_h, gate_ref, bins_ref,
    grad_ref, gg_ref, loss_ref,
    attn_v, w_v, resid_v, target_v, err, psend, precv,
    at_send, at, dp, gbuf, ra, sb, rb, cnt, lpart, lbuf,
    ld, fs, fr, a_s, a_r, p_s, p_r, c_s, c_r, l_s, l_r, lp_s, lp_r,
    dx_s, dx_r, dy_s, dy_r, fx_s, fx_r, fy_s, fy_r, za_s, za_r, zb_s, zb_r,
):
    d = lax.axis_index("dp")
    mp = lax.axis_index("mp")
    other = 1 - mp
    x = lax.rem(d, 2)
    y = lax.rem(lax.div(d, 2), 2)
    q = lax.rem(d, PLANE)
    b0 = lax.rem(lax.div(d, PLANE), 2)
    b1 = lax.div(d, 2 * PLANE)
    x_q = q + 1 - 2 * x
    y_q = q + 2 - 4 * y
    xy_q = x_q + 2 - 4 * y
    base = d - q
    x_dev, y_dev, xy_dev = (base + x_q, mp), (base + y_q, mp), (base + xy_q, mp)
    za_dev = (d + PLANE - 2 * PLANE * b0, mp)
    zb_dev = (d + 2 * PLANE - 4 * PLANE * b1, mp)
    partner = (d, other)

    rows, own_cols = attn_v.shape
    samples = gate_ref.shape[0]
    tok = rows // samples
    nb = dp.shape[1]
    nf, _, fw = psend.shape
    chunk = grad_ref.shape[0]
    half = rows // 2

    def remote(src, dst, send, recv, dev):
        return pltpu.make_async_remote_copy(
            src_ref=src, dst_ref=dst, send_sem=send, recv_sem=recv, device_id=dev, device_id_type=MESH
        )

    def own_half(which):
        return w_h.at[:, pl.ds(pl.multiple_of(which * own_cols, LANES), own_cols)]

    loads = [
        pltpu.make_async_copy(attn_h, attn_v, ld.at[0]),
        pltpu.make_async_copy(own_half(other), w_v.at[0], ld.at[1]),
        pltpu.make_async_copy(own_half(mp), w_v.at[1], ld.at[2]),
        pltpu.make_async_copy(resid_h, resid_v, ld.at[3]),
        pltpu.make_async_copy(target_h, target_v, ld.at[4]),
    ]
    for load in loads:
        load.start()

    barrier = pltpu.get_barrier_semaphore()
    for k in range(1, n):
        pl.semaphore_signal(barrier, inc=1, device_id=(lax.rem(d + k, n), mp), device_id_type=MESH)
    pl.semaphore_signal(barrier, inc=1, device_id=partner, device_id_type=MESH)

    lane = lax.broadcasted_iota(jnp.int32, (8, LANES), 1)
    one_hot = [(lane == bins_ref[s]).astype(jnp.float32) for s in range(samples)]
    counts_own = one_hot[0]
    for s in range(1, samples):
        counts_own = counts_own + one_hot[s]
    cnt[d] = counts_own

    loads[0].wait()
    turned = attn_v[...].T
    for k in range(own_cols // chunk):
        zz, to = k // PLANE, k % PLANE
        at_send[to, zz * chunk:(zz + 1) * chunk, :] = turned[k * chunk:(k + 1) * chunk]

    pl.semaphore_wait(barrier, n)

    count_copies = []
    for k in range(1, n):
        copy = remote(cnt.at[d], cnt.at[d], c_s.at[k], c_r.at[k], (lax.rem(d + k, n), mp))
        copy.start()
        count_copies.append(copy)
    attn_copies = []
    for r, (peer_q, dev) in enumerate(((xy_q, xy_dev), (x_q, x_dev), (y_q, y_dev))):
        copy = remote(at_send.at[peer_q], at.at[q, mp], a_s.at[r], a_r.at[r], dev)
        copy.start()
        attn_copies.append(copy)
    partner_copies = [remote(at_send.at[q], at.at[q, mp], p_s.at[3], p_r.at[3], partner)]
    partner_copies[0].start()
    at[q, mp] = at_send[q]

    loads[1].wait()
    part_copies = []
    for j in range(nf):
        cols = slice(j * fw, (j + 1) * fw)
        psend[j] = jnp.dot(attn_v[...], w_v[0, :, cols], preferred_element_type=jnp.float32)
        copy = remote(psend.at[j], precv.at[j], fs.at[j], fr.at[j], partner)
        copy.start()
        part_copies.append(copy)
    loads[2].wait()
    loads[3].wait()
    loads[4].wait()
    square = [jnp.zeros((1, fw), jnp.float32) for _ in range(samples)]
    gate_sums = []
    for j in range(nf):
        cols = slice(j * fw, (j + 1) * fw)
        own = jnp.dot(attn_v[...], w_v[1, :, cols], preferred_element_type=jnp.float32)
        part_copies[j].wait_recv()
        sums = []
        for s in range(samples):
            toks = slice(s * tok, (s + 1) * tok)
            proj = own[toks] + precv[j, toks, :]
            gate = gate_ref[s:s + 1, cols]
            hidden = resid_v[toks, cols].astype(jnp.float32) + gate * proj
            error = hidden - target_v[toks, cols].astype(jnp.float32)
            err[toks, cols] = error
            square[s] = square[s] + jnp.sum(error * error, axis=0, keepdims=True)
            sums.append(jnp.sum(error * proj, axis=0, keepdims=True))
        gate_sums.append(sums)

    bin_part = jnp.zeros((8, LANES), jnp.float32)
    for s in range(samples):
        sample_error = jnp.sum(square[s], axis=1, keepdims=True) / (tok * full_width)
        bin_part = bin_part + one_hot[s] * sample_error
    lpart[mp] = bin_part
    loss_pair = remote(lpart.at[mp], lpart.at[mp], lp_s.at[0], lp_r.at[0], partner)
    loss_pair.start()

    centre = (lane.astype(jnp.float32) + 0.5) / LANES
    logit = jnp.log(centre) - jnp.log(1.0 - centre)
    weights = jnp.exp(-0.5 * logit * logit) / (math.sqrt(2.0 * math.pi) * centre * (1.0 - centre))

    for copy in count_copies:
        copy.wait_recv()
    counts = cnt[0]
    for k in range(1, n):
        counts = counts + cnt[k]
    floored = jnp.maximum(counts, 1.0)
    scale_bin = LOSS_SCALE * weights / floored
    coef = [
        jnp.sum((one_hot[s] * scale_bin)[0:1], axis=1, keepdims=True) * (2.0 / (tok * full_width))
        for s in range(samples)
    ]

    def make_d_proj(c):
        cols = slice(c * LANES, (c + 1) * LANES)
        for s in range(samples):
            toks = slice(s * tok, (s + 1) * tok)
            d_hidden = coef[s] * err[toks, cols]
            dp[q, c, toks, :] = (d_hidden * gate_ref[s:s + 1, cols]).astype(jnp.bfloat16)

    direct_x = [remote(dp.at[q, c], dp.at[q, c], dx_s.at[c], dx_r.at[c], x_dev) for c in range(nb)]
    direct_y = [remote(dp.at[q, c], dp.at[q, c], dy_s.at[c], dy_r.at[c], y_dev) for c in range(nb)]
    first, second = pl.ds(0, half), pl.ds(half, half)
    pass_y = [
        remote(dp.at[x_q, c, first], dp.at[x_q, c, first], fy_s.at[c], fy_r.at[c], y_dev)
        for c in range(nb)
    ]
    pass_x = [
        remote(dp.at[y_q, c, second], dp.at[y_q, c, second], fx_s.at[c], fx_r.at[c], x_dev)
        for c in range(nb)
    ]
    halve_a = [remote(gbuf.at[c, 1 - b0], ra.at[c], za_s.at[c], za_r.at[c], za_dev) for c in range(nb)]
    halve_b = [remote(sb.at[c], rb.at[c], zb_s.at[c], zb_r.at[c], zb_dev) for c in range(nb)]

    def start_direct(c):
        direct_x[c].start()
        direct_y[c].start()

    def multiply(c):
        pass_x[c].wait_recv()
        pass_y[c].wait_recv()
        total = jnp.dot(
            at[0].reshape(PLANE * chunk, rows), dp[0, c], preferred_element_type=jnp.float32
        )
        for p in range(1, PLANE):
            total = total + jnp.dot(
                at[p].reshape(PLANE * chunk, rows), dp[p, c], preferred_element_type=jnp.float32
            )
        for m in range(2):
            for zz in range(2):
                k = 2 * m + zz
                gbuf[c, zz, m] = total[k * chunk:(k + 1) * chunk]
        halve_a[c].start()

    def reduce_a(c):
        halve_a[c].wait_recv()
        sb[c] = gbuf[c, b0, 1 - b1] + ra[c, 1 - b1]
        halve_b[c].start()

    def reduce_b(c):
        halve_b[c].wait_recv()
        grad_ref[:, c * LANES:(c + 1) * LANES] = (gbuf[c, b0, b1] + ra[c, b1]) + rb[c]

    ahead = 2
    for c in range(nb):
        make_d_proj(c)
        if c < ahead:
            start_direct(c)

    for r, peer_q in enumerate((xy_q, x_q, y_q)):
        attn_copies[r].wait_recv()
        copy = remote(at.at[peer_q, mp], at.at[peer_q, mp], p_s.at[r], p_r.at[r], partner)
        copy.start()
        partner_copies.append(copy)

    for j in range(nf):
        cols = slice(j * fw, (j + 1) * fw)
        for s in range(samples):
            gg_ref[s:s + 1, cols] = coef[s] * gate_sums[j][s]
    loss_pair.wait_recv()
    lbuf[d] = lpart[0] + lpart[1]
    loss_copies = []
    for k in range(1, n):
        copy = remote(lbuf.at[d], lbuf.at[d], l_s.at[k], l_r.at[k], (lax.rem(d + k, n), mp))
        copy.start()
        loss_copies.append(copy)

    for step in range(nb + 3):
        if step < nb:
            direct_x[step].wait_recv()
            pass_y[step].start()
            direct_y[step].wait_recv()
            pass_x[step].start()
            if step + ahead < nb:
                start_direct(step + ahead)
        if step == 1:
            for copy in partner_copies:
                copy.wait_recv()
        if 1 <= step <= nb:
            multiply(step - 1)
        if 2 <= step <= nb + 1:
            reduce_a(step - 2)
        if 3 <= step:
            reduce_b(step - 3)

    for copy in loss_copies:
        copy.wait_recv()
    sums = lbuf[0]
    for k in range(1, n):
        sums = sums + lbuf[k]
    loss_ref[...] = (weights * sums / floored)[0:1]

    for group in (
        count_copies, attn_copies, partner_copies, part_copies, [loss_pair], loss_copies,
        direct_x, direct_y, pass_x, pass_y, halve_a, halve_b,
    ):
        for copy in group:
            copy.wait_send()


def fused(n, attn, w_out, resid, target, gate, bins):
    rows, own_cols = attn.shape
    samples = bins.shape[0]
    full_width = w_out.shape[1]
    chunk = full_width // n
    nb = own_cols // LANES
    fw = 2 * LANES if own_cols % (2 * LANES) == 0 else LANES
    nf = own_cols // fw
    f32, bf16 = jnp.float32, jnp.bfloat16
    V = pltpu.VMEM
    dma = pltpu.SemaphoreType.DMA
    grad, gate_grad, loss = pl.pallas_call(
        functools.partial(fused_kernel, n, full_width),
        out_shape=(
            jax.ShapeDtypeStruct((chunk, own_cols), f32),
            jax.ShapeDtypeStruct((samples, own_cols), f32),
            jax.ShapeDtypeStruct((1, NBINS), f32),
        ),
        in_specs=[pl.BlockSpec(memory_space=pl.ANY)] * 4
        + [pl.BlockSpec(memory_space=pltpu.VMEM), pl.BlockSpec(memory_space=pltpu.SMEM)],
        out_specs=(pl.BlockSpec(memory_space=pltpu.VMEM),) * 3,
        scratch_shapes=[
            V((rows, own_cols), bf16),
            V((2, w_out.shape[0], own_cols), bf16),
            V((rows, own_cols), bf16),
            V((rows, own_cols), bf16),
            V((rows, own_cols), f32),
            V((nf, rows, fw), f32),
            V((nf, rows, fw), f32),
            V((PLANE, 2 * chunk, rows), bf16),
            V((PLANE, 2, 2 * chunk, rows), bf16),
            V((PLANE, nb, rows, LANES), bf16),
            V((nb, 2, 2, chunk, LANES), f32),
            V((nb, 2, chunk, LANES), f32),
            V((nb, chunk, LANES), f32),
            V((nb, chunk, LANES), f32),
            V((n, 8, LANES), f32),
            V((2, 8, LANES), f32),
            V((n, 8, LANES), f32),
            dma((5,)),
            dma((nf,)), dma((nf,)),
            dma((3,)), dma((3,)),
            dma((4,)), dma((4,)),
            dma((n,)), dma((n,)),
            dma((n,)), dma((n,)),
            dma((1,)), dma((1,)),
        ] + [dma((nb,))] * 12,
        compiler_params=pltpu.CompilerParams(collective_id=0, has_side_effects=True),
    )(attn, w_out, resid, target, gate, bins)
    return grad, gate_grad, loss.reshape(NBINS)


def solution(mesh):
    n, pair = mesh.shape["dp"], mesh.shape["mp"]

    def body(attn, w_out, resid, target, gate, bins):
        full_width = w_out.shape[1]
        fits = (
            pair == 2 and n == PLANE * 4 and NBINS == LANES
            and full_width % (16 * n) == 0 and attn.shape[1] % LANES == 0
            and attn.shape[0] % (16 * bins.shape[0]) == 0 and attn.shape[0] % LANES == 0
        )
        if fits:
            return fused(n, attn, w_out, resid, target, gate, bins)
        return shards(attn, w_out, resid, target, gate, bins)

    return jax.shard_map(
        body,
        mesh=mesh,
        in_specs=(
            P("dp", "mp"),
            P("mp", None),
            P("dp", "mp"),
            P("dp", "mp"),
            P("dp", "mp"),
            P("dp"),
        ),
        out_specs=(P("dp", "mp"), P("dp", "mp"), P()),
        check_vma=False,
    )
```

```python
import functools
import math

import jax
import jax.numpy as jnp
from jax import lax
from jax.experimental import pallas as pl
from jax.experimental.pallas import tpu as pltpu
from jax.sharding import PartitionSpec as P

NBINS = 128


LOSS_SCALE = 4096.0


def bin_weights():
    centre = (jnp.arange(NBINS).astype(jnp.float32) + 0.5) / NBINS
    logit = jnp.log(centre) - jnp.log(1.0 - centre)
    return jnp.exp(-0.5 * logit * logit) / (math.sqrt(2.0 * math.pi) * centre * (1.0 - centre))


def shards(attn, w_out, resid, target, gate, bins):
    samples = bins.shape[0]
    tok_rows = attn.shape[0]
    per_sample = tok_rows // samples
    full_width = w_out.shape[1]
    own_cols = resid.shape[1]
    bin_ids = jnp.arange(NBINS, dtype=jnp.int32)
    one_hot = (bins[:, None] == bin_ids[None, :]).astype(jnp.float32)
    local_counts = jnp.sum(one_hot, axis=0)
    weights = bin_weights()
    counts = lax.psum(local_counts, "dp")
    whole_attn = lax.all_gather(attn, "mp", axis=1, tiled=True)
    partial_value = jnp.dot(attn, w_out, preferred_element_type=jnp.float32)
    projected = lax.psum_scatter(partial_value, "mp", scatter_dimension=1, tiled=True)
    proj_cube = projected.reshape(samples, per_sample, own_cols)
    hidden = (
        resid.reshape(samples, per_sample, own_cols).astype(jnp.float32)
        + gate[:, None, :] * proj_cube
    )
    error_cube = hidden - target.reshape(samples, per_sample, own_cols).astype(jnp.float32)
    sample_error = jnp.sum(error_cube * error_cube, axis=(1, 2)) / (per_sample * full_width)
    bin_part = jnp.sum(one_hot * sample_error[:, None], axis=0)
    sums = lax.psum(bin_part, ("dp", "mp"))
    floored = jnp.maximum(counts, 1.0)
    scale_bin = LOSS_SCALE * weights / floored
    coefficient = jnp.sum(one_hot * scale_bin[None, :], axis=1) * (2.0 / (per_sample * full_width))
    d_hidden = coefficient[:, None, None] * error_cube
    grad_gate = jnp.sum(d_hidden * proj_cube, axis=1)
    d_proj = (d_hidden * gate[:, None, :]).astype(jnp.bfloat16).reshape(tok_rows, own_cols)
    full_grad = lax.dot_general(
        whole_attn, d_proj, (((0,), (0,)), ((), ())), preferred_element_type=jnp.float32
    )
    grad_out = lax.psum_scatter(full_grad, "dp", scatter_dimension=0, tiled=True)
    bin_loss = weights * sums / floored
    return (grad_out, grad_gate, bin_loss)


MESH = pl.DeviceIdType.MESH
LANES = 128
PLANE = 4


def fused_kernel(
    n, full_width,
    attn_h, w_h, resid_h, target_h, gate_h, bins_h,
    grad_ref, gg_ref, loss_ref,
    attn_v, w_v, resid_v, target_v, gate_ref, bins_ref, err, psend, precv,
    at_send, at, dp, gbuf, ra, sb, rb, lpart, cnt, cline, lbuf, lline,
    ld, fs, fr, a_s, a_r, p_s, p_r, c_s, c_r, l_s, l_r, lp_s, lp_r,
    dx_s, dx_r, dy_s, dy_r, fx_s, fx_r, fy_s, fy_r, za_s, za_r, zk_s, zk_r, zb_s, zb_r,
):
    d = lax.axis_index("dp")
    mp = lax.axis_index("mp")
    other = 1 - mp
    x = lax.rem(d, 2)
    y = lax.rem(lax.div(d, 2), 2)
    q = lax.rem(d, PLANE)
    b0 = lax.rem(lax.div(d, PLANE), 2)
    b1 = lax.div(d, 2 * PLANE)
    x_q = q + 1 - 2 * x
    y_q = q + 2 - 4 * y
    xy_q = x_q + 2 - 4 * y
    base = d - q
    x_dev, y_dev, xy_dev = (base + x_q, mp), (base + y_q, mp), (base + xy_q, mp)
    za_dev = (d + PLANE - 2 * PLANE * b0, mp)
    zb_dev = (d + 2 * PLANE - 4 * PLANE * b1, mp)
    partner = (d, other)

    rows, own_cols = attn_v.shape
    samples = gate_ref.shape[0]
    tok = rows // samples
    nb = dp.shape[1]
    nf, _, fw = psend.shape
    chunk = grad_ref.shape[0]
    half = rows // 2

    def remote(src, dst, send, recv, dev):
        return pltpu.make_async_remote_copy(
            src_ref=src, dst_ref=dst, send_sem=send, recv_sem=recv, device_id=dev, device_id_type=MESH
        )

    def own_half(which):
        return w_h.at[:, pl.ds(pl.multiple_of(which * own_cols, LANES), own_cols)]

    loads = [
        pltpu.make_async_copy(attn_h, attn_v, ld.at[0]),
        pltpu.make_async_copy(own_half(other), w_v.at[0], ld.at[1]),
        pltpu.make_async_copy(own_half(mp), w_v.at[1], ld.at[2]),
        pltpu.make_async_copy(resid_h, resid_v, ld.at[3]),
        pltpu.make_async_copy(target_h, target_v, ld.at[4]),
        pltpu.make_async_copy(bins_h, bins_ref, ld.at[5]),
        pltpu.make_async_copy(gate_h, gate_ref, ld.at[6]),
    ]

    barrier = pltpu.get_barrier_semaphore()
    peers = (zb_dev, xy_dev, za_dev, x_dev, y_dev, partner)
    for peer in peers:
        pl.semaphore_signal(barrier, inc=1, device_id=peer, device_id_type=MESH)

    for load in loads:
        load.start()
    loads[5].wait()
    lane = lax.broadcasted_iota(jnp.int32, (8, LANES), 1)
    one_hot = [(lane == bins_ref[s]).astype(jnp.float32) for s in range(samples)]
    counts_own = one_hot[0]
    for s in range(1, samples):
        counts_own = counts_own + one_hot[s]
    cnt[q] = counts_own

    loads[0].wait()
    turned = attn_v[...].T
    for k in range(own_cols // chunk):
        zz, to = k // PLANE, k % PLANE
        at_send[to, zz * chunk:(zz + 1) * chunk, :] = turned[k * chunk:(k + 1) * chunk]

    pl.semaphore_wait(barrier, len(peers))

    count_copies = []
    plane = (xy_dev, x_dev, y_dev)
    for r, dev in enumerate(plane):
        copy = remote(cnt.at[q], cnt.at[q], c_s.at[r], c_r.at[r], dev)
        copy.start()
        count_copies.append(copy)
    attn_copies = []
    for r, (peer_q, dev) in enumerate(((xy_q, xy_dev), (x_q, x_dev), (y_q, y_dev))):
        copy = remote(at_send.at[peer_q], at.at[q, mp], a_s.at[r], a_r.at[r], dev)
        copy.start()
        attn_copies.append(copy)
    partner_copies = [remote(at_send.at[q], at.at[q, mp], p_s.at[3], p_r.at[3], partner)]
    partner_copies[0].start()
    at[q, mp] = at_send[q]

    loads[1].wait()
    part_copies = []
    for j in range(nf):
        cols = slice(j * fw, (j + 1) * fw)
        psend[j] = jnp.dot(attn_v[...], w_v[0, :, cols], preferred_element_type=jnp.float32)
        copy = remote(psend.at[j], precv.at[j], fs.at[j], fr.at[j], partner)
        copy.start()
        part_copies.append(copy)
    def line_step(copies, line, values, sends, recvs, stage, dev):
        line[2 * stage] = values
        copy = remote(line.at[2 * stage], line.at[2 * stage + 1], sends.at[3 + stage], recvs.at[3 + stage], dev)
        copy.start()
        copies.append(copy)

    for copy in count_copies:
        copy.wait_recv()
    line_step(count_copies, cline, (cnt[0] + cnt[1]) + (cnt[2] + cnt[3]), c_s, c_r, 0, za_dev)
    for load in loads[2:5]:
        load.wait()
    loads[6].wait()
    square = [jnp.zeros((1, fw), jnp.float32) for _ in range(samples)]
    gate_sums = []
    for j in range(nf):
        cols = slice(j * fw, (j + 1) * fw)
        own = jnp.dot(attn_v[...], w_v[1, :, cols], preferred_element_type=jnp.float32)
        part_copies[j].wait_recv()
        sums = []
        for s in range(samples):
            toks = slice(s * tok, (s + 1) * tok)
            proj = own[toks] + precv[j, toks, :]
            gate = gate_ref[s:s + 1, cols]
            hidden = resid_v[toks, cols].astype(jnp.float32) + gate * proj
            error = hidden - target_v[toks, cols].astype(jnp.float32)
            err[toks, cols] = error
            square[s] = square[s] + jnp.sum(error * error, axis=0, keepdims=True)
            sums.append(jnp.sum(error * proj, axis=0, keepdims=True))
        gate_sums.append(sums)
        if j == 0:
            count_copies[3].wait_recv()
            line_step(count_copies, cline, cline[0] + cline[1], c_s, c_r, 1, zb_dev)

    bin_part = jnp.zeros((8, LANES), jnp.float32)
    for s in range(samples):
        sample_error = jnp.sum(square[s], axis=1, keepdims=True) / (tok * full_width)
        bin_part = bin_part + one_hot[s] * sample_error
    lpart[mp] = bin_part
    loss_pair = remote(lpart.at[mp], lpart.at[mp], lp_s.at[0], lp_r.at[0], partner)
    loss_pair.start()

    centre = (lane.astype(jnp.float32) + 0.5) / LANES
    logit = jnp.log(centre) - jnp.log(1.0 - centre)
    weights = jnp.exp(-0.5 * logit * logit) / (math.sqrt(2.0 * math.pi) * centre * (1.0 - centre))

    count_copies[4].wait_recv()
    counts = cline[2] + cline[3]
    floored = jnp.maximum(counts, 1.0)
    scale_bin = LOSS_SCALE * weights / floored
    coef = [
        jnp.sum((one_hot[s] * scale_bin)[0:1], axis=1, keepdims=True) * (2.0 / (tok * full_width))
        for s in range(samples)
    ]

    def make_d_proj(c):
        cols = slice(c * LANES, (c + 1) * LANES)
        for s in range(samples):
            toks = slice(s * tok, (s + 1) * tok)
            d_hidden = coef[s] * err[toks, cols]
            dp[q, c, toks, :] = (d_hidden * gate_ref[s:s + 1, cols]).astype(jnp.bfloat16)

    direct_x = [remote(dp.at[q, c], dp.at[q, c], dx_s.at[c], dx_r.at[c], x_dev) for c in range(nb)]
    direct_y = [remote(dp.at[q, c], dp.at[q, c], dy_s.at[c], dy_r.at[c], y_dev) for c in range(nb)]
    first, second = pl.ds(0, half), pl.ds(half, half)
    pass_y = [
        remote(dp.at[x_q, c, first], dp.at[x_q, c, first], fy_s.at[c], fy_r.at[c], y_dev)
        for c in range(nb)
    ]
    pass_x = [
        remote(dp.at[y_q, c, second], dp.at[y_q, c, second], fx_s.at[c], fx_r.at[c], x_dev)
        for c in range(nb)
    ]
    halve_a = [
        remote(gbuf.at[c, 1 - b0, 1 - b1], ra.at[c, 0], za_s.at[c], za_r.at[c], za_dev) for c in range(nb)
    ]
    halve_k = [
        remote(gbuf.at[c, 1 - b0, b1], ra.at[c, 1], zk_s.at[c], zk_r.at[c], za_dev) for c in range(nb)
    ]
    halve_b = [remote(sb.at[c], rb.at[c], zb_s.at[c], zb_r.at[c], zb_dev) for c in range(nb)]

    def start_direct(c):
        direct_x[c].start()
        direct_y[c].start()

    def multiply(c):
        pass_x[c].wait_recv()
        pass_y[c].wait_recv()
        total = jnp.dot(
            at[0].reshape(PLANE * chunk, rows), dp[0, c], preferred_element_type=jnp.float32
        )
        for p in range(1, PLANE):
            total = total + jnp.dot(
                at[p].reshape(PLANE * chunk, rows), dp[p, c], preferred_element_type=jnp.float32
            )
        for m in range(2):
            for zz in range(2):
                k = 2 * m + zz
                gbuf[c, zz, m] = total[k * chunk:(k + 1) * chunk]
        halve_a[c].start()
        halve_k[c].start()

    def reduce_a(c):
        halve_a[c].wait_recv()
        sb[c] = gbuf[c, b0, 1 - b1] + ra[c, 0]
        halve_b[c].start()

    def reduce_b(c):
        halve_k[c].wait_recv()
        halve_b[c].wait_recv()
        grad_ref[:, c * LANES:(c + 1) * LANES] = (gbuf[c, b0, b1] + ra[c, 1]) + rb[c]

    ahead = 2
    for c in range(nb):
        make_d_proj(c)
        if c < ahead:
            start_direct(c)

    for r, peer_q in enumerate((xy_q, x_q, y_q)):
        attn_copies[r].wait_recv()
        copy = remote(at.at[peer_q, mp], at.at[peer_q, mp], p_s.at[r], p_r.at[r], partner)
        copy.start()
        partner_copies.append(copy)

    for j in range(nf):
        cols = slice(j * fw, (j + 1) * fw)
        for s in range(samples):
            gg_ref[s:s + 1, cols] = coef[s] * gate_sums[j][s]
    loss_pair.wait_recv()
    lbuf[q] = lpart[0] + lpart[1]
    loss_copies = []
    for r, dev in enumerate(plane):
        copy = remote(lbuf.at[q], lbuf.at[q], l_s.at[r], l_r.at[r], dev)
        copy.start()
        loss_copies.append(copy)

    for step in range(nb + 3):
        if step < nb:
            direct_x[step].wait_recv()
            pass_y[step].start()
            direct_y[step].wait_recv()
            pass_x[step].start()
            if step + ahead < nb:
                start_direct(step + ahead)
        if step == 1:
            for copy in partner_copies:
                copy.wait_recv()
        if 1 <= step <= nb:
            multiply(step - 1)
        if step == 2:
            for copy in loss_copies:
                copy.wait_recv()
            line_step(loss_copies, lline, (lbuf[0] + lbuf[1]) + (lbuf[2] + lbuf[3]), l_s, l_r, 0, za_dev)
        if step == 4:
            loss_copies[3].wait_recv()
            line_step(loss_copies, lline, lline[0] + lline[1], l_s, l_r, 1, zb_dev)
        if 2 <= step <= nb + 1:
            reduce_a(step - 2)
        if 3 <= step:
            reduce_b(step - 3)

    loss_copies[4].wait_recv()
    sums = lline[2] + lline[3]
    loss_ref[...] = (weights * sums / floored)[0:1]

    for group in (
        count_copies, attn_copies, partner_copies, part_copies, [loss_pair], loss_copies,
        direct_x, direct_y, pass_x, pass_y, halve_a, halve_k, halve_b,
    ):
        for copy in group:
            copy.wait_send()


def fused(n, attn, w_out, resid, target, gate, bins):
    rows, own_cols = attn.shape
    samples = bins.shape[0]
    full_width = w_out.shape[1]
    chunk = full_width // n
    nb = own_cols // LANES
    fw = 2 * LANES if own_cols % (2 * LANES) == 0 else LANES
    nf = own_cols // fw
    f32, bf16 = jnp.float32, jnp.bfloat16
    V = pltpu.VMEM
    dma = pltpu.SemaphoreType.DMA
    grad, gate_grad, loss = pl.pallas_call(
        functools.partial(fused_kernel, n, full_width),
        out_shape=(
            jax.ShapeDtypeStruct((chunk, own_cols), f32),
            jax.ShapeDtypeStruct((samples, own_cols), f32),
            jax.ShapeDtypeStruct((1, NBINS), f32),
        ),
        in_specs=[pl.BlockSpec(memory_space=pl.ANY)] * 6,
        out_specs=(pl.BlockSpec(memory_space=pltpu.VMEM),) * 3,
        scratch_shapes=[
            V((rows, own_cols), bf16),
            V((2, w_out.shape[0], own_cols), bf16),
            V((rows, own_cols), bf16),
            V((rows, own_cols), bf16),
            V((samples, own_cols), f32),
            pltpu.SMEM((samples,), jnp.int32),
            V((rows, own_cols), f32),
            V((nf, rows, fw), f32),
            V((nf, rows, fw), f32),
            V((PLANE, 2 * chunk, rows), bf16),
            V((PLANE, 2, 2 * chunk, rows), bf16),
            V((PLANE, nb, rows, LANES), bf16),
            V((nb, 2, 2, chunk, LANES), f32),
            V((nb, 2, chunk, LANES), f32),
            V((nb, chunk, LANES), f32),
            V((nb, chunk, LANES), f32),
            V((2, 8, LANES), f32),
            V((PLANE, 8, LANES), f32),
            V((PLANE, 8, LANES), f32),
            V((PLANE, 8, LANES), f32),
            V((PLANE, 8, LANES), f32),
            dma((7,)),
            dma((nf,)), dma((nf,)),
            dma((3,)), dma((3,)),
            dma((4,)), dma((4,)),
            dma((5,)), dma((5,)),
            dma((5,)), dma((5,)),
            dma((1,)), dma((1,)),
        ] + [dma((nb,))] * 14,
        compiler_params=pltpu.CompilerParams(collective_id=0, has_side_effects=True),
    )(attn, w_out, resid, target, gate, bins)
    return grad, gate_grad, loss.reshape(NBINS)


def solution(mesh):
    n, pair = mesh.shape["dp"], mesh.shape["mp"]

    def body(attn, w_out, resid, target, gate, bins):
        full_width = w_out.shape[1]
        fits = (
            pair == 2 and n == PLANE * 4 and NBINS == LANES
            and full_width % (16 * n) == 0 and attn.shape[1] % LANES == 0
            and attn.shape[0] % (16 * bins.shape[0]) == 0 and attn.shape[0] % LANES == 0
        )
        if fits:
            return fused(n, attn, w_out, resid, target, gate, bins)
        return shards(attn, w_out, resid, target, gate, bins)

    return jax.shard_map(
        body,
        mesh=mesh,
        in_specs=(
            P("dp", "mp"),
            P("mp", None),
            P("dp", "mp"),
            P("dp", "mp"),
            P("dp", "mp"),
            P("dp"),
        ),
        out_specs=(P("dp", "mp"), P("dp", "mp"), P()),
        check_vma=False,
    )
```

```python
import functools
import math

import jax
import jax.numpy as jnp
from jax import lax
from jax.experimental import pallas as pl
from jax.experimental.pallas import tpu as pltpu
from jax.sharding import PartitionSpec as P

NBINS = 128


LOSS_SCALE = 4096.0


def bin_weights():
    centre = (jnp.arange(NBINS).astype(jnp.float32) + 0.5) / NBINS
    logit = jnp.log(centre) - jnp.log(1.0 - centre)
    return jnp.exp(-0.5 * logit * logit) / (math.sqrt(2.0 * math.pi) * centre * (1.0 - centre))


def shards(attn, w_out, resid, target, gate, bins):
    samples = bins.shape[0]
    tok_rows = attn.shape[0]
    per_sample = tok_rows // samples
    full_width = w_out.shape[1]
    own_cols = resid.shape[1]
    bin_ids = jnp.arange(NBINS, dtype=jnp.int32)
    one_hot = (bins[:, None] == bin_ids[None, :]).astype(jnp.float32)
    local_counts = jnp.sum(one_hot, axis=0)
    weights = bin_weights()
    counts = lax.psum(local_counts, "dp")
    whole_attn = lax.all_gather(attn, "mp", axis=1, tiled=True)
    partial_value = jnp.dot(attn, w_out, preferred_element_type=jnp.float32)
    projected = lax.psum_scatter(partial_value, "mp", scatter_dimension=1, tiled=True)
    proj_cube = projected.reshape(samples, per_sample, own_cols)
    hidden = (
        resid.reshape(samples, per_sample, own_cols).astype(jnp.float32)
        + gate[:, None, :] * proj_cube
    )
    error_cube = hidden - target.reshape(samples, per_sample, own_cols).astype(jnp.float32)
    sample_error = jnp.sum(error_cube * error_cube, axis=(1, 2)) / (per_sample * full_width)
    bin_part = jnp.sum(one_hot * sample_error[:, None], axis=0)
    sums = lax.psum(bin_part, ("dp", "mp"))
    floored = jnp.maximum(counts, 1.0)
    scale_bin = LOSS_SCALE * weights / floored
    coefficient = jnp.sum(one_hot * scale_bin[None, :], axis=1) * (2.0 / (per_sample * full_width))
    d_hidden = coefficient[:, None, None] * error_cube
    grad_gate = jnp.sum(d_hidden * proj_cube, axis=1)
    d_proj = (d_hidden * gate[:, None, :]).astype(jnp.bfloat16).reshape(tok_rows, own_cols)
    full_grad = lax.dot_general(
        whole_attn, d_proj, (((0,), (0,)), ((), ())), preferred_element_type=jnp.float32
    )
    grad_out = lax.psum_scatter(full_grad, "dp", scatter_dimension=0, tiled=True)
    bin_loss = weights * sums / floored
    return (grad_out, grad_gate, bin_loss)


MESH = pl.DeviceIdType.MESH
LANES = 128
PLANE = 4


def fused_kernel(
    n, full_width,
    attn_h, w_h, resid_h, target_h, gate_h, bins_h,
    grad_ref, gg_ref, loss_ref,
    attn_v, w_v, resid_v, target_v, gate_ref, bins_ref, err, psend, precv, own_part,
    at_send, at, dp, gbuf, ra, sb, rb, lpart, cnt, cline, lbuf, lline,
    ld, fs, fr, a_s, a_r, p_s, p_r, c_s, c_r, l_s, l_r, lp_s, lp_r,
    dx_s, dx_r, dy_s, dy_r, fx_s, fx_r, fy_s, fy_r, za_s, za_r, zk_s, zk_r, zb_s, zb_r,
):
    d = lax.axis_index("dp")
    mp = lax.axis_index("mp")
    other = 1 - mp
    x = lax.rem(d, 2)
    y = lax.rem(lax.div(d, 2), 2)
    q = lax.rem(d, PLANE)
    b0 = lax.rem(lax.div(d, PLANE), 2)
    b1 = lax.div(d, 2 * PLANE)
    x_q = q + 1 - 2 * x
    y_q = q + 2 - 4 * y
    xy_q = x_q + 2 - 4 * y
    base = d - q
    x_dev, y_dev, xy_dev = (base + x_q, mp), (base + y_q, mp), (base + xy_q, mp)
    za_dev = (d + PLANE - 2 * PLANE * b0, mp)
    zb_dev = (d + 2 * PLANE - 4 * PLANE * b1, mp)
    zab_dev = (d + PLANE - 2 * PLANE * b0 + 2 * PLANE - 4 * PLANE * b1, mp)
    z = lax.div(d, PLANE)
    partner = (d, other)

    rows, own_cols = attn_v.shape
    samples = gate_ref.shape[0]
    tok = rows // samples
    nb = dp.shape[1]
    nf, _, fw = psend.shape
    chunk = grad_ref.shape[0]
    half = rows // 2

    def remote(src, dst, send, recv, dev):
        return pltpu.make_async_remote_copy(
            src_ref=src, dst_ref=dst, send_sem=send, recv_sem=recv, device_id=dev, device_id_type=MESH
        )

    def own_half(which):
        return w_h.at[:, pl.ds(pl.multiple_of(which * own_cols, LANES), own_cols)]

    loads = [
        pltpu.make_async_copy(attn_h, attn_v, ld.at[0]),
        pltpu.make_async_copy(own_half(other), w_v.at[0], ld.at[1]),
        pltpu.make_async_copy(own_half(mp), w_v.at[1], ld.at[2]),
        pltpu.make_async_copy(resid_h, resid_v, ld.at[3]),
        pltpu.make_async_copy(target_h, target_v, ld.at[4]),
        pltpu.make_async_copy(bins_h, bins_ref, ld.at[5]),
        pltpu.make_async_copy(gate_h, gate_ref, ld.at[6]),
    ]

    barrier = pltpu.get_barrier_semaphore()
    peers = (zab_dev, zb_dev, xy_dev, za_dev, x_dev, y_dev, partner)
    for peer in peers:
        pl.semaphore_signal(barrier, inc=1, device_id=peer, device_id_type=MESH)

    loads[0].start()
    loads[5].start()
    loads[5].wait()
    lane = lax.broadcasted_iota(jnp.int32, (8, LANES), 1)
    one_hot = [(lane == bins_ref[s]).astype(jnp.float32) for s in range(samples)]
    counts_own = one_hot[0]
    for s in range(1, samples):
        counts_own = counts_own + one_hot[s]
    cnt[q] = counts_own

    pl.semaphore_wait(barrier, len(peers))

    count_copies = []
    plane = (xy_dev, x_dev, y_dev)
    for r, dev in enumerate(plane):
        copy = remote(cnt.at[q], cnt.at[q], c_s.at[r], c_r.at[r], dev)
        copy.start()
        count_copies.append(copy)
    loads[0].wait()
    for k in (1, 2, 6, 3, 4):
        loads[k].start()
    turned = attn_v[...].T
    for k in range(own_cols // chunk):
        zz, to = k // PLANE, k % PLANE
        at_send[to, zz * chunk:(zz + 1) * chunk, :] = turned[k * chunk:(k + 1) * chunk]

    attn_copies = []
    for r, (peer_q, dev) in enumerate(((xy_q, xy_dev), (x_q, x_dev), (y_q, y_dev))):
        copy = remote(at_send.at[peer_q], at.at[q, mp], a_s.at[r], a_r.at[r], dev)
        copy.start()
        attn_copies.append(copy)
    partner_copies = [remote(at_send.at[q], at.at[q, mp], p_s.at[3], p_r.at[3], partner)]
    partner_copies[0].start()
    at[q, mp] = at_send[q]

    loads[1].wait()
    part_copies = []
    for j in range(nf):
        cols = slice(j * fw, (j + 1) * fw)
        psend[j] = jnp.dot(attn_v[...], w_v[0, :, cols], preferred_element_type=jnp.float32)
        copy = remote(psend.at[j], precv.at[j], fs.at[j], fr.at[j], partner)
        copy.start()
        part_copies.append(copy)
    def line_step(copies, line, values, sends, recvs, stage, dev):
        line[2 * stage] = values
        copy = remote(line.at[2 * stage], line.at[2 * stage + 1], sends.at[3 + stage], recvs.at[3 + stage], dev)
        copy.start()
        copies.append(copy)

    loads[2].wait()
    for j in range(nf):
        own_part[j] = jnp.dot(
            attn_v[...], w_v[1, :, j * fw:(j + 1) * fw], preferred_element_type=jnp.float32
        )
    for copy in count_copies:
        copy.wait_recv()
    cline[z] = (cnt[0] + cnt[1]) + (cnt[2] + cnt[3])
    for r, dev in enumerate((zab_dev, zb_dev, za_dev)):
        copy = remote(cline.at[z], cline.at[z], c_s.at[3 + r], c_r.at[3 + r], dev)
        copy.start()
        count_copies.append(copy)
    for load in loads[3:5]:
        load.wait()
    loads[6].wait()
    square = [jnp.zeros((1, fw), jnp.float32) for _ in range(samples)]
    gate_sums = []
    for j in range(nf):
        cols = slice(j * fw, (j + 1) * fw)
        part_copies[j].wait_recv()
        sums = []
        for s in range(samples):
            toks = slice(s * tok, (s + 1) * tok)
            proj = own_part[j, toks, :] + precv[j, toks, :]
            gate = gate_ref[s:s + 1, cols]
            hidden = resid_v[toks, cols].astype(jnp.float32) + gate * proj
            error = hidden - target_v[toks, cols].astype(jnp.float32)
            err[toks, cols] = error
            square[s] = square[s] + jnp.sum(error * error, axis=0, keepdims=True)
            sums.append(jnp.sum(error * proj, axis=0, keepdims=True))
        gate_sums.append(sums)

    bin_part = jnp.zeros((8, LANES), jnp.float32)
    for s in range(samples):
        sample_error = jnp.sum(square[s], axis=1, keepdims=True) / (tok * full_width)
        bin_part = bin_part + one_hot[s] * sample_error
    lpart[mp] = bin_part
    loss_pair = remote(lpart.at[mp], lpart.at[mp], lp_s.at[0], lp_r.at[0], partner)
    loss_pair.start()

    centre = (lane.astype(jnp.float32) + 0.5) / LANES
    logit = jnp.log(centre) - jnp.log(1.0 - centre)
    weights = jnp.exp(-0.5 * logit * logit) / (math.sqrt(2.0 * math.pi) * centre * (1.0 - centre))

    for copy in count_copies[3:]:
        copy.wait_recv()
    counts = (cline[0] + cline[1]) + (cline[2] + cline[3])
    floored = jnp.maximum(counts, 1.0)
    scale_bin = LOSS_SCALE * weights / floored
    coef = [
        jnp.sum((one_hot[s] * scale_bin)[0:1], axis=1, keepdims=True) * (2.0 / (tok * full_width))
        for s in range(samples)
    ]

    def make_d_proj(c):
        cols = slice(c * LANES, (c + 1) * LANES)
        for s in range(samples):
            toks = slice(s * tok, (s + 1) * tok)
            d_hidden = coef[s] * err[toks, cols]
            dp[q, c, toks, :] = (d_hidden * gate_ref[s:s + 1, cols]).astype(jnp.bfloat16)

    direct_x = [remote(dp.at[q, c], dp.at[q, c], dx_s.at[c], dx_r.at[c], x_dev) for c in range(nb)]
    direct_y = [remote(dp.at[q, c], dp.at[q, c], dy_s.at[c], dy_r.at[c], y_dev) for c in range(nb)]
    first, second = pl.ds(0, half), pl.ds(half, half)
    pass_y = [
        remote(dp.at[x_q, c, first], dp.at[x_q, c, first], fy_s.at[c], fy_r.at[c], y_dev)
        for c in range(nb)
    ]
    pass_x = [
        remote(dp.at[y_q, c, second], dp.at[y_q, c, second], fx_s.at[c], fx_r.at[c], x_dev)
        for c in range(nb)
    ]
    halve_a = [
        remote(gbuf.at[c, 1 - b0, 1 - b1], ra.at[c, 0], za_s.at[c], za_r.at[c], za_dev) for c in range(nb)
    ]
    halve_k = [
        remote(gbuf.at[c, 1 - b0, b1], ra.at[c, 1], zk_s.at[c], zk_r.at[c], za_dev) for c in range(nb)
    ]
    halve_b = [remote(sb.at[c], rb.at[c], zb_s.at[c], zb_r.at[c], zb_dev) for c in range(nb)]

    def start_direct(c):
        direct_x[c].start()
        direct_y[c].start()

    def multiply(c):
        def product(p):
            return jnp.dot(
                at[p].reshape(PLANE * chunk, rows), dp[p, c], preferred_element_type=jnp.float32
            )

        near = product(q) + product(x_q) + product(y_q)
        pass_x[c].wait_recv()
        pass_y[c].wait_recv()
        total = near + product(xy_q)
        for m in range(2):
            for zz in range(2):
                k = 2 * m + zz
                gbuf[c, zz, m] = total[k * chunk:(k + 1) * chunk]
        halve_a[c].start()
        halve_k[c].start()

    def reduce_a(c):
        halve_a[c].wait_recv()
        sb[c] = gbuf[c, b0, 1 - b1] + ra[c, 0]
        halve_b[c].start()

    def reduce_b(c):
        halve_k[c].wait_recv()
        halve_b[c].wait_recv()
        grad_ref[:, c * LANES:(c + 1) * LANES] = (gbuf[c, b0, b1] + ra[c, 1]) + rb[c]

    ahead = 2
    for c in range(nb):
        make_d_proj(c)
        if c < ahead:
            start_direct(c)

    for r, peer_q in enumerate((xy_q, x_q, y_q)):
        attn_copies[r].wait_recv()
        copy = remote(at.at[peer_q, mp], at.at[peer_q, mp], p_s.at[r], p_r.at[r], partner)
        copy.start()
        partner_copies.append(copy)

    for j in range(nf):
        cols = slice(j * fw, (j + 1) * fw)
        for s in range(samples):
            gg_ref[s:s + 1, cols] = coef[s] * gate_sums[j][s]
    loss_pair.wait_recv()
    lbuf[q] = lpart[0] + lpart[1]
    loss_copies = []
    for r, dev in enumerate(plane):
        copy = remote(lbuf.at[q], lbuf.at[q], l_s.at[r], l_r.at[r], dev)
        copy.start()
        loss_copies.append(copy)

    for step in range(nb + 3):
        if step < nb:
            direct_x[step].wait_recv()
            pass_y[step].start()
            direct_y[step].wait_recv()
            pass_x[step].start()
            if step + ahead < nb:
                start_direct(step + ahead)
        if step == 1:
            for copy in partner_copies:
                copy.wait_recv()
        if 1 <= step <= nb:
            multiply(step - 1)
        if step == 2:
            for copy in loss_copies:
                copy.wait_recv()
            line_step(loss_copies, lline, (lbuf[0] + lbuf[1]) + (lbuf[2] + lbuf[3]), l_s, l_r, 0, za_dev)
        if step == 4:
            loss_copies[3].wait_recv()
            line_step(loss_copies, lline, lline[0] + lline[1], l_s, l_r, 1, zb_dev)
        if 2 <= step <= nb + 1:
            reduce_a(step - 2)
        if 3 <= step:
            reduce_b(step - 3)

    loss_copies[4].wait_recv()
    sums = lline[2] + lline[3]
    loss_ref[...] = (weights * sums / floored)[0:1]

    for group in (
        count_copies, attn_copies, partner_copies, part_copies, [loss_pair], loss_copies,
        direct_x, direct_y, pass_x, pass_y, halve_a, halve_k, halve_b,
    ):
        for copy in group:
            copy.wait_send()


def hand_over(*refs):
    for k in range(3):
        refs[k + 3][...] = refs[k][...]


def fused(n, attn, w_out, resid, target, gate, bins):
    rows, own_cols = attn.shape
    samples = bins.shape[0]
    full_width = w_out.shape[1]
    chunk = full_width // n
    nb = own_cols // LANES
    fw = 2 * LANES if own_cols % (2 * LANES) == 0 else LANES
    nf = own_cols // fw
    f32, bf16 = jnp.float32, jnp.bfloat16
    V = pltpu.VMEM
    dma = pltpu.SemaphoreType.DMA
    grad, gate_grad, loss = pl.pallas_call(
        functools.partial(fused_kernel, n, full_width),
        out_shape=(
            jax.ShapeDtypeStruct((chunk, own_cols), f32),
            jax.ShapeDtypeStruct((samples, own_cols), f32),
            jax.ShapeDtypeStruct((1, NBINS), f32),
        ),
        in_specs=[pl.BlockSpec(memory_space=pl.ANY)] * 6,
        out_specs=(pl.BlockSpec(memory_space=pltpu.VMEM),) * 3,
        scratch_shapes=[
            V((rows, own_cols), bf16),
            V((2, w_out.shape[0], own_cols), bf16),
            V((rows, own_cols), bf16),
            V((rows, own_cols), bf16),
            V((samples, own_cols), f32),
            pltpu.SMEM((samples,), jnp.int32),
            V((rows, own_cols), f32),
            V((nf, rows, fw), f32),
            V((nf, rows, fw), f32),
            V((nf, rows, fw), f32),
            V((PLANE, 2 * chunk, rows), bf16),
            V((PLANE, 2, 2 * chunk, rows), bf16),
            V((PLANE, nb, rows, LANES), bf16),
            V((nb, 2, 2, chunk, LANES), f32),
            V((nb, 2, chunk, LANES), f32),
            V((nb, chunk, LANES), f32),
            V((nb, chunk, LANES), f32),
            V((2, 8, LANES), f32),
            V((PLANE, 8, LANES), f32),
            V((PLANE, 8, LANES), f32),
            V((PLANE, 8, LANES), f32),
            V((PLANE, 8, LANES), f32),
            dma((7,)),
            dma((nf,)), dma((nf,)),
            dma((3,)), dma((3,)),
            dma((4,)), dma((4,)),
            dma((6,)), dma((6,)),
            dma((5,)), dma((5,)),
            dma((1,)), dma((1,)),
        ] + [dma((nb,))] * 14,
        compiler_params=pltpu.CompilerParams(collective_id=0, has_side_effects=True),
    )(attn, w_out, resid, target, gate, bins)
    vmem = pl.BlockSpec(memory_space=pltpu.VMEM)
    grad, gate_grad, loss = pl.pallas_call(
        hand_over,
        out_shape=tuple(jax.ShapeDtypeStruct(a.shape, f32) for a in (grad, gate_grad, loss)),
        in_specs=[vmem] * 3,
        out_specs=(vmem,) * 3,
    )(grad, gate_grad, loss)
    return grad, gate_grad, loss.reshape(NBINS)


def solution(mesh):
    n, pair = mesh.shape["dp"], mesh.shape["mp"]

    def body(attn, w_out, resid, target, gate, bins):
        full_width = w_out.shape[1]
        fits = (
            pair == 2 and n == PLANE * 4 and NBINS == LANES
            and full_width % (16 * n) == 0 and attn.shape[1] % LANES == 0
            and attn.shape[0] % (16 * bins.shape[0]) == 0 and attn.shape[0] % LANES == 0
        )
        if fits:
            return fused(n, attn, w_out, resid, target, gate, bins)
        return shards(attn, w_out, resid, target, gate, bins)

    return jax.shard_map(
        body,
        mesh=mesh,
        in_specs=(
            P("dp", "mp"),
            P("mp", None),
            P("dp", "mp"),
            P("dp", "mp"),
            P("dp", "mp"),
            P("dp"),
        ),
        out_specs=(P("dp", "mp"), P("dp", "mp"), P()),
        check_vma=False,
    )
```

```python
import functools
import math

import jax
import jax.numpy as jnp
from jax import lax
from jax.experimental import pallas as pl
from jax.experimental.pallas import tpu as pltpu
from jax.sharding import PartitionSpec as P

NBINS = 128


LOSS_SCALE = 4096.0


def bin_weights():
    centre = (jnp.arange(NBINS).astype(jnp.float32) + 0.5) / NBINS
    logit = jnp.log(centre) - jnp.log(1.0 - centre)
    return jnp.exp(-0.5 * logit * logit) / (math.sqrt(2.0 * math.pi) * centre * (1.0 - centre))


def shards(attn, w_out, resid, target, gate, bins):
    samples = bins.shape[0]
    tok_rows = attn.shape[0]
    per_sample = tok_rows // samples
    full_width = w_out.shape[1]
    own_cols = resid.shape[1]
    bin_ids = jnp.arange(NBINS, dtype=jnp.int32)
    one_hot = (bins[:, None] == bin_ids[None, :]).astype(jnp.float32)
    local_counts = jnp.sum(one_hot, axis=0)
    weights = bin_weights()
    counts = lax.psum(local_counts, "dp")
    whole_attn = lax.all_gather(attn, "mp", axis=1, tiled=True)
    partial_value = jnp.dot(attn, w_out, preferred_element_type=jnp.float32)
    projected = lax.psum_scatter(partial_value, "mp", scatter_dimension=1, tiled=True)
    proj_cube = projected.reshape(samples, per_sample, own_cols)
    hidden = (
        resid.reshape(samples, per_sample, own_cols).astype(jnp.float32)
        + gate[:, None, :] * proj_cube
    )
    error_cube = hidden - target.reshape(samples, per_sample, own_cols).astype(jnp.float32)
    sample_error = jnp.sum(error_cube * error_cube, axis=(1, 2)) / (per_sample * full_width)
    bin_part = jnp.sum(one_hot * sample_error[:, None], axis=0)
    sums = lax.psum(bin_part, ("dp", "mp"))
    floored = jnp.maximum(counts, 1.0)
    scale_bin = LOSS_SCALE * weights / floored
    coefficient = jnp.sum(one_hot * scale_bin[None, :], axis=1) * (2.0 / (per_sample * full_width))
    d_hidden = coefficient[:, None, None] * error_cube
    grad_gate = jnp.sum(d_hidden * proj_cube, axis=1)
    d_proj = (d_hidden * gate[:, None, :]).astype(jnp.bfloat16).reshape(tok_rows, own_cols)
    full_grad = lax.dot_general(
        whole_attn, d_proj, (((0,), (0,)), ((), ())), preferred_element_type=jnp.float32
    )
    grad_out = lax.psum_scatter(full_grad, "dp", scatter_dimension=0, tiled=True)
    bin_loss = weights * sums / floored
    return (grad_out, grad_gate, bin_loss)


MESH = pl.DeviceIdType.MESH
LANES = 128
PLANE = 4


def fused_kernel(
    n, full_width,
    attn_h, w_h, resid_h, target_h, gate_h, bins_h,
    grad_ref, gg_ref, loss_ref,
    attn_v, w_v, resid_v, target_v, gate_ref, bins_ref, err, psend, precv, own_part,
    at_send, at, dp, gbuf, ra, sb, rb, lpart, cnt, cline, lbuf, lline,
    ld, fs, fr, a_s, a_r, p_s, p_r, c_s, c_r, l_s, l_r, lp_s, lp_r,
    dx_s, dx_r, dy_s, dy_r, ex_s, ex_r, ey_s, ey_r, fx_s, fx_r, fy_s, fy_r, za_s, za_r, zk_s, zk_r, zb_s, zb_r,
):
    d = lax.axis_index("dp")
    mp = lax.axis_index("mp")
    other = 1 - mp
    x = lax.rem(d, 2)
    y = lax.rem(lax.div(d, 2), 2)
    q = lax.rem(d, PLANE)
    b0 = lax.rem(lax.div(d, PLANE), 2)
    b1 = lax.div(d, 2 * PLANE)
    x_q = q + 1 - 2 * x
    y_q = q + 2 - 4 * y
    xy_q = x_q + 2 - 4 * y
    base = d - q
    x_dev, y_dev, xy_dev = (base + x_q, mp), (base + y_q, mp), (base + xy_q, mp)
    za_dev = (d + PLANE - 2 * PLANE * b0, mp)
    zb_dev = (d + 2 * PLANE - 4 * PLANE * b1, mp)
    zab_dev = (d + PLANE - 2 * PLANE * b0 + 2 * PLANE - 4 * PLANE * b1, mp)
    z = lax.div(d, PLANE)
    partner = (d, other)

    rows, own_cols = attn_v.shape
    samples = gate_ref.shape[0]
    tok = rows // samples
    nb = dp.shape[1]
    nf, _, fw = psend.shape
    chunk = grad_ref.shape[0]
    half = rows // 2

    def remote(src, dst, send, recv, dev):
        return pltpu.make_async_remote_copy(
            src_ref=src, dst_ref=dst, send_sem=send, recv_sem=recv, device_id=dev, device_id_type=MESH
        )

    def own_half(which):
        return w_h.at[:, pl.ds(pl.multiple_of(which * own_cols, LANES), own_cols)]

    loads = [
        pltpu.make_async_copy(attn_h, attn_v, ld.at[0]),
        pltpu.make_async_copy(own_half(other), w_v.at[0], ld.at[1]),
        pltpu.make_async_copy(own_half(mp), w_v.at[1], ld.at[2]),
        pltpu.make_async_copy(resid_h, resid_v, ld.at[3]),
        pltpu.make_async_copy(target_h, target_v, ld.at[4]),
        pltpu.make_async_copy(bins_h, bins_ref, ld.at[5]),
        pltpu.make_async_copy(gate_h, gate_ref, ld.at[6]),
    ]

    barrier = pltpu.get_barrier_semaphore()
    peers = (zab_dev, zb_dev, xy_dev, za_dev, x_dev, y_dev, partner)
    for peer in peers:
        pl.semaphore_signal(barrier, inc=1, device_id=peer, device_id_type=MESH)

    loads[0].start()
    loads[5].start()
    loads[5].wait()
    lane = lax.broadcasted_iota(jnp.int32, (8, LANES), 1)
    one_hot = [(lane == bins_ref[s]).astype(jnp.float32) for s in range(samples)]
    counts_own = one_hot[0]
    for s in range(1, samples):
        counts_own = counts_own + one_hot[s]
    cnt[q] = counts_own

    pl.semaphore_wait(barrier, len(peers))

    count_copies = []
    plane = (xy_dev, x_dev, y_dev)
    for r, dev in enumerate(plane):
        copy = remote(cnt.at[q], cnt.at[q], c_s.at[r], c_r.at[r], dev)
        copy.start()
        count_copies.append(copy)
    loads[0].wait()
    for k in (1, 2, 6, 3, 4):
        loads[k].start()
    turned = attn_v[...].T
    for k in range(own_cols // chunk):
        zz, to = k // PLANE, k % PLANE
        at_send[to, zz * chunk:(zz + 1) * chunk, :] = turned[k * chunk:(k + 1) * chunk]

    attn_copies = []
    for r, (peer_q, dev) in enumerate(((xy_q, xy_dev), (x_q, x_dev), (y_q, y_dev))):
        copy = remote(at_send.at[peer_q], at.at[q, mp], a_s.at[r], a_r.at[r], dev)
        copy.start()
        attn_copies.append(copy)
    partner_copies = [remote(at_send.at[q], at.at[q, mp], p_s.at[3], p_r.at[3], partner)]
    partner_copies[0].start()
    at[q, mp] = at_send[q]

    loads[1].wait()
    part_copies = []
    for j in range(nf):
        cols = slice(j * fw, (j + 1) * fw)
        psend[j] = jnp.dot(attn_v[...], w_v[0, :, cols], preferred_element_type=jnp.float32)
        copy = remote(psend.at[j], precv.at[j], fs.at[j], fr.at[j], partner)
        copy.start()
        part_copies.append(copy)
    def line_step(copies, line, values, sends, recvs, stage, dev):
        line[2 * stage] = values
        copy = remote(line.at[2 * stage], line.at[2 * stage + 1], sends.at[3 + stage], recvs.at[3 + stage], dev)
        copy.start()
        copies.append(copy)

    loads[2].wait()
    for j in range(nf):
        own_part[j] = jnp.dot(
            attn_v[...], w_v[1, :, j * fw:(j + 1) * fw], preferred_element_type=jnp.float32
        )
    for copy in count_copies:
        copy.wait_recv()
    cline[z] = (cnt[0] + cnt[1]) + (cnt[2] + cnt[3])
    for r, dev in enumerate((zab_dev, zb_dev, za_dev)):
        copy = remote(cline.at[z], cline.at[z], c_s.at[3 + r], c_r.at[3 + r], dev)
        copy.start()
        count_copies.append(copy)
    for load in loads[3:5]:
        load.wait()
    loads[6].wait()
    square = [jnp.zeros((1, fw), jnp.float32) for _ in range(samples)]
    gate_sums = []
    for j in range(nf):
        cols = slice(j * fw, (j + 1) * fw)
        part_copies[j].wait_recv()
        sums = []
        for s in range(samples):
            toks = slice(s * tok, (s + 1) * tok)
            proj = own_part[j, toks, :] + precv[j, toks, :]
            gate = gate_ref[s:s + 1, cols]
            hidden = resid_v[toks, cols].astype(jnp.float32) + gate * proj
            error = hidden - target_v[toks, cols].astype(jnp.float32)
            err[toks, cols] = error
            square[s] = square[s] + jnp.sum(error * error, axis=0, keepdims=True)
            sums.append(jnp.sum(error * proj, axis=0, keepdims=True))
        gate_sums.append(sums)

    bin_part = jnp.zeros((8, LANES), jnp.float32)
    for s in range(samples):
        sample_error = jnp.sum(square[s], axis=1, keepdims=True) / (tok * full_width)
        bin_part = bin_part + one_hot[s] * sample_error
    lpart[mp] = bin_part
    loss_pair = remote(lpart.at[mp], lpart.at[mp], lp_s.at[0], lp_r.at[0], partner)
    loss_pair.start()

    centre = (lane.astype(jnp.float32) + 0.5) / LANES
    logit = jnp.log(centre) - jnp.log(1.0 - centre)
    weights = jnp.exp(-0.5 * logit * logit) / (math.sqrt(2.0 * math.pi) * centre * (1.0 - centre))

    for copy in count_copies[3:]:
        copy.wait_recv()
    counts = (cline[0] + cline[1]) + (cline[2] + cline[3])
    floored = jnp.maximum(counts, 1.0)
    scale_bin = LOSS_SCALE * weights / floored
    coef = [
        jnp.sum((one_hot[s] * scale_bin)[0:1], axis=1, keepdims=True) * (2.0 / (tok * full_width))
        for s in range(samples)
    ]

    def make_d_proj(c):
        cols = slice(c * LANES, (c + 1) * LANES)
        for s in range(samples):
            toks = slice(s * tok, (s + 1) * tok)
            d_hidden = coef[s] * err[toks, cols]
            dp[q, c, toks, :] = (d_hidden * gate_ref[s:s + 1, cols]).astype(jnp.bfloat16)

    first, second = pl.ds(0, half), pl.ds(half, half)

    def direct(part, sends, recvs, dev):
        return [
            remote(dp.at[q, c, part], dp.at[q, c, part], sends.at[c], recvs.at[c], dev) for c in range(nb)
        ]

    direct_x = direct(first, dx_s, dx_r, x_dev)
    direct_y = direct(second, dy_s, dy_r, y_dev)
    rest_x = direct(second, ex_s, ex_r, x_dev)
    rest_y = direct(first, ey_s, ey_r, y_dev)
    pass_y = [
        remote(dp.at[x_q, c, first], dp.at[x_q, c, first], fy_s.at[c], fy_r.at[c], y_dev)
        for c in range(nb)
    ]
    pass_x = [
        remote(dp.at[y_q, c, second], dp.at[y_q, c, second], fx_s.at[c], fx_r.at[c], x_dev)
        for c in range(nb)
    ]
    halve_a = [
        remote(gbuf.at[c, 1 - b0, 1 - b1], ra.at[c, 0], za_s.at[c], za_r.at[c], za_dev) for c in range(nb)
    ]
    halve_k = [
        remote(gbuf.at[c, 1 - b0, b1], ra.at[c, 1], zk_s.at[c], zk_r.at[c], za_dev) for c in range(nb)
    ]
    halve_b = [remote(sb.at[c], rb.at[c], zb_s.at[c], zb_r.at[c], zb_dev) for c in range(nb)]

    def start_direct(c):
        direct_x[c].start()
        direct_y[c].start()
        rest_x[c].start()
        rest_y[c].start()

    def multiply(c):
        def product(p, m):
            return jnp.dot(at[p, m], dp[p, c], preferred_element_type=jnp.float32)

        halves = (1 - b1, b1)
        near = [product(q, m) for m in halves]
        rest_x[c].wait_recv()
        rest_y[c].wait_recv()
        near = [near[k] + product(x_q, m) + product(y_q, m) for k, m in enumerate(halves)]
        pass_x[c].wait_recv()
        pass_y[c].wait_recv()
        for k, m in enumerate(halves):
            total = near[k] + product(xy_q, m)
            for zz in range(2):
                gbuf[c, zz, m] = total[zz * chunk:(zz + 1) * chunk]
            (halve_a, halve_k)[k][c].start()

    def reduce_a(c):
        halve_a[c].wait_recv()
        sb[c] = gbuf[c, b0, 1 - b1] + ra[c, 0]
        halve_b[c].start()

    def reduce_b(c):
        halve_k[c].wait_recv()
        halve_b[c].wait_recv()
        grad_ref[:, c * LANES:(c + 1) * LANES] = (gbuf[c, b0, b1] + ra[c, 1]) + rb[c]

    ahead = 2
    for c in range(nb):
        make_d_proj(c)
        if c < ahead:
            start_direct(c)

    for r, peer_q in enumerate((xy_q, x_q, y_q)):
        attn_copies[r].wait_recv()
        copy = remote(at.at[peer_q, mp], at.at[peer_q, mp], p_s.at[r], p_r.at[r], partner)
        copy.start()
        partner_copies.append(copy)

    for j in range(nf):
        cols = slice(j * fw, (j + 1) * fw)
        for s in range(samples):
            gg_ref[s:s + 1, cols] = coef[s] * gate_sums[j][s]
    loss_pair.wait_recv()
    lbuf[q] = lpart[0] + lpart[1]
    loss_copies = []
    for r, dev in enumerate(plane):
        copy = remote(lbuf.at[q], lbuf.at[q], l_s.at[r], l_r.at[r], dev)
        copy.start()
        loss_copies.append(copy)

    for step in range(nb + 3):
        if step < nb:
            direct_x[step].wait_recv()
            pass_y[step].start()
            direct_y[step].wait_recv()
            pass_x[step].start()
            if step + ahead < nb:
                start_direct(step + ahead)
        if step == 1:
            for copy in partner_copies:
                copy.wait_recv()
        if 1 <= step <= nb:
            multiply(step - 1)
        if step == 2:
            for copy in loss_copies:
                copy.wait_recv()
            line_step(loss_copies, lline, (lbuf[0] + lbuf[1]) + (lbuf[2] + lbuf[3]), l_s, l_r, 0, za_dev)
        if step == 4:
            loss_copies[3].wait_recv()
            line_step(loss_copies, lline, lline[0] + lline[1], l_s, l_r, 1, zb_dev)
        if 2 <= step <= nb + 1:
            reduce_a(step - 2)
        if 3 <= step:
            reduce_b(step - 3)

    loss_copies[4].wait_recv()
    sums = lline[2] + lline[3]
    loss_ref[...] = (weights * sums / floored)[0:1]

    for group in (
        count_copies, attn_copies, partner_copies, part_copies, [loss_pair], loss_copies,
        direct_x, direct_y, rest_x, rest_y, pass_x, pass_y, halve_a, halve_k, halve_b,
    ):
        for copy in group:
            copy.wait_send()


def hand_over(*refs):
    for k in range(3):
        refs[k + 3][...] = refs[k][...]


def fused(n, attn, w_out, resid, target, gate, bins):
    rows, own_cols = attn.shape
    samples = bins.shape[0]
    full_width = w_out.shape[1]
    chunk = full_width // n
    nb = own_cols // LANES
    fw = 2 * LANES if own_cols % (2 * LANES) == 0 else LANES
    nf = own_cols // fw
    f32, bf16 = jnp.float32, jnp.bfloat16
    V = pltpu.VMEM
    dma = pltpu.SemaphoreType.DMA
    grad, gate_grad, loss = pl.pallas_call(
        functools.partial(fused_kernel, n, full_width),
        out_shape=(
            jax.ShapeDtypeStruct((chunk, own_cols), f32),
            jax.ShapeDtypeStruct((samples, own_cols), f32),
            jax.ShapeDtypeStruct((1, NBINS), f32),
        ),
        in_specs=[pl.BlockSpec(memory_space=pl.ANY)] * 6,
        out_specs=(pl.BlockSpec(memory_space=pltpu.VMEM),) * 3,
        scratch_shapes=[
            V((rows, own_cols), bf16),
            V((2, w_out.shape[0], own_cols), bf16),
            V((rows, own_cols), bf16),
            V((rows, own_cols), bf16),
            V((samples, own_cols), f32),
            pltpu.SMEM((samples,), jnp.int32),
            V((rows, own_cols), f32),
            V((nf, rows, fw), f32),
            V((nf, rows, fw), f32),
            V((nf, rows, fw), f32),
            V((PLANE, 2 * chunk, rows), bf16),
            V((PLANE, 2, 2 * chunk, rows), bf16),
            V((PLANE, nb, rows, LANES), bf16),
            V((nb, 2, 2, chunk, LANES), f32),
            V((nb, 2, chunk, LANES), f32),
            V((nb, chunk, LANES), f32),
            V((nb, chunk, LANES), f32),
            V((2, 8, LANES), f32),
            V((PLANE, 8, LANES), f32),
            V((PLANE, 8, LANES), f32),
            V((PLANE, 8, LANES), f32),
            V((PLANE, 8, LANES), f32),
            dma((7,)),
            dma((nf,)), dma((nf,)),
            dma((3,)), dma((3,)),
            dma((4,)), dma((4,)),
            dma((6,)), dma((6,)),
            dma((5,)), dma((5,)),
            dma((1,)), dma((1,)),
        ] + [dma((nb,))] * 18,
        compiler_params=pltpu.CompilerParams(collective_id=0, has_side_effects=True),
    )(attn, w_out, resid, target, gate, bins)
    vmem = pl.BlockSpec(memory_space=pltpu.VMEM)
    grad, gate_grad, loss = pl.pallas_call(
        hand_over,
        out_shape=tuple(jax.ShapeDtypeStruct(a.shape, f32) for a in (grad, gate_grad, loss)),
        in_specs=[vmem] * 3,
        out_specs=(vmem,) * 3,
    )(grad, gate_grad, loss)
    return grad, gate_grad, loss.reshape(NBINS)


def solution(mesh):
    n, pair = mesh.shape["dp"], mesh.shape["mp"]

    def body(attn, w_out, resid, target, gate, bins):
        full_width = w_out.shape[1]
        fits = (
            pair == 2 and n == PLANE * 4 and NBINS == LANES
            and full_width % (16 * n) == 0 and attn.shape[1] % LANES == 0
            and attn.shape[0] % (16 * bins.shape[0]) == 0 and attn.shape[0] % LANES == 0
        )
        if fits:
            return fused(n, attn, w_out, resid, target, gate, bins)
        return shards(attn, w_out, resid, target, gate, bins)

    return jax.shard_map(
        body,
        mesh=mesh,
        in_specs=(
            P("dp", "mp"),
            P("mp", None),
            P("dp", "mp"),
            P("dp", "mp"),
            P("dp", "mp"),
            P("dp"),
        ),
        out_specs=(P("dp", "mp"), P("dp", "mp"), P()),
        check_vma=False,
    )
```
